256 devices in a mesh: rows: 8 (over z_hi, y), cols: 16 (over z_lo, x_lo, core), shift: 2 (over x_hi).
Axes of the slice: x: 4 (x_hi: 2, x_lo: 2; x = x_hi * 2 + x_lo), y: 4, z: 8 (z_hi: 2, z_lo: 4; z = z_hi * 4 + z_lo), core: 2. Of those that a mesh axis runs over, the one named last changes fastest.
Arguments:
- train_gate: bfloat16 [7168, 14336], P(('shift', 'rows'), 'cols'), parts along dimension 0, may hold values from -0.09375 to 0.09375
- low_gate: bfloat16 [7168, 64], P(('shift', 'rows')), parts along dimension 0, may hold values from -0.09375 to 0.09375
- high_gate: bfloat16 [128, 14336], P('shift', 'cols'), parts along dimension 0, may hold values from -0.75 to 0.75
- train_up: bfloat16 [7168, 14336], P(('shift', 'rows'), 'cols'), parts along dimension 0, may hold values from -0.09375 to 0.09375
- low_up: bfloat16 [7168, 64], P(('shift', 'rows')), parts along dimension 0, may hold values from -0.09375 to 0.09375
- high_up: bfloat16 [128, 14336], P('shift', 'cols'), parts along dimension 0, may hold values from -0.75 to 0.75
- train_down: bfloat16 [28672, 3584], P(('shift', 'cols'), 'rows'), parts along dimension 0, may hold values from -0.046875 to 0.046875
- low_down: bfloat16 [28672, 64], P(('shift', 'cols')), parts along dimension 0, may hold values from -0.046875 to 0.046875
- high_down: bfloat16 [128, 3584], P('shift', 'rows'), parts along dimension 0, may hold values from -0.75 to 0.75
- norm_train: float32 [7168], P(('shift', 'rows', 'cols')), parts along dimension 0, may hold values from 0.25 to 1.75
- norm_step: float32 [7168], P(('shift', 'rows', 'cols')), parts along dimension 0, may hold values from -0.3 to 0.3
Outputs:
- serving_gate: bfloat16 [28672, 3584], P(('shift', 'cols')), parts along dimension 0
- serving_up: bfloat16 [28672, 3584], P(('shift', 'cols')), parts along dimension 0
- serving_down: bfloat16 [7168, 14336], P('shift', 'cols'), parts along dimension 0
- serve_norm: bfloat16 [7168], P('shift'), parts along dimension 0
The draws below stay inside these ranges and needn't reach their ends.
There are 2 independent parts, one for each index of `shift`. The reference program is written for one: setup_inputs(seed, part) draws one part's arguments, and reference() takes and returns one part's arrays. A program takes and returns all parts, laid end to end along the dimension named above; each array names one. Nothing has to cross between parts.
All inputs are finite; a program needn't handle non-finite values.
Results may differ from the reference program's by a relative error of at most 0.001.
Values may be sent and summed in bfloat16 or wider, within the bound.
No kernel may reach another device: no remote copies, remote signals or barrier semaphores. Data moves between devices by JAX's collectives and lax.ppermute only.
A program may use at most 128 MiB of HBM per device.

```python
import jax
import jax.numpy as jnp

D_MODEL = 3584
D_INNER = 14336
RANK = 64


def shard_levels(rng, shape, shards, least, top_value):
    gain = 1.0
    for dim, blocks in shards:
        steps = jax.random.uniform(jax.random.fold_in(jax.random.fold_in(rng, 6), dim), (blocks,), jnp.float32, least / len(shards), top_value / len(shards))
        gain = gain * jnp.repeat(jnp.exp(steps), shape[dim] // blocks).reshape((-1,) + (1,) * (len(shape) - 1 - dim))
    return gain


def noise(rng, extent, deviation, reach, shards=(), dtype=jnp.bfloat16):
    array = deviation * jax.random.normal(rng, extent, jnp.float32)
    if shards:
        array = array * shard_levels(rng, extent, shards, -0.22, 0.18)
    return jnp.clip(array, -reach, reach).astype(dtype)


def setup_inputs(seed: int = 0, part: int = 0) -> dict:
    key_list = jax.random.split(jax.random.key(seed), 12)
    part_keys = jax.random.split(jax.random.fold_in(key_list[11], part), 12)
    return {
        "train_gate": noise(part_keys[0], (D_MODEL, D_INNER), D_MODEL ** -0.5, 0.09375, ((0, 8), (1, 16))),
        "low_gate": noise(part_keys[1], (D_MODEL, RANK), D_MODEL ** -0.5, 0.09375, ((0, 8),)),
        "high_gate": noise(part_keys[2], (RANK, D_INNER), RANK ** -0.5, 0.75, ((1, 16),)),
        "train_up": noise(part_keys[3], (D_MODEL, D_INNER), D_MODEL ** -0.5, 0.09375, ((0, 8), (1, 16))),
        "low_up": noise(part_keys[4], (D_MODEL, RANK), D_MODEL ** -0.5, 0.09375, ((0, 8),)),
        "high_up": noise(part_keys[5], (RANK, D_INNER), RANK ** -0.5, 0.75, ((1, 16),)),
        "train_down": noise(part_keys[6], (D_INNER, D_MODEL), D_INNER ** -0.5, 0.046875, ((0, 16), (1, 8))),
        "low_down": noise(part_keys[7], (D_INNER, RANK), D_INNER ** -0.5, 0.046875, ((0, 16),)),
        "high_down": noise(part_keys[8], (RANK, D_MODEL), RANK ** -0.5, 0.75, ((1, 8),)),
        "norm_train": jnp.clip(1.0 + 0.15 * jax.random.normal(part_keys[9], (D_MODEL,), jnp.float32), 0.25, 1.75),
        "norm_step": jnp.clip(jax.random.uniform(part_keys[10], (D_MODEL,), jnp.float32, -0.3, 0.3) * shard_levels(part_keys[10], (D_MODEL,), ((0, 128),), -0.4, 0.0), -0.3, 0.3),
    }


mix_rate = 1.0


def reference(train_gate, low_gate, high_gate, train_up, low_up, high_up, train_down, low_down, high_down, norm_train, norm_step):
    whole_gate = train_gate.astype(jnp.float32) + mix_rate * jnp.dot(low_gate, high_gate, preferred_element_type=jnp.float32)
    whole_up = train_up.astype(jnp.float32) + mix_rate * jnp.dot(low_up, high_up, preferred_element_type=jnp.float32)
    whole_down = train_down.astype(jnp.float32) + mix_rate * jnp.dot(low_down, high_down, preferred_element_type=jnp.float32)
    serving_gate = whole_gate.T.astype(jnp.bfloat16)
    serving_up = whole_up.T.astype(jnp.bfloat16)
    serving_down = whole_down.T.astype(jnp.bfloat16)
    serve_norm = (norm_train + norm_step).astype(jnp.bfloat16)
    return serving_gate, serving_up, serving_down, serve_norm
```

```python
import functools

import jax
import jax.numpy as jnp
from jax import lax
from jax.experimental import pallas as pl
from jax.experimental.pallas import tpu as pltpu
from jax.sharding import Mesh
from jax.sharding import PartitionSpec as P

ROWS = ("zh", "y")
COLS = ("zl", "xl", "core")
mix_rate = 1.0


RING = 4
UP = [(i, (i + 1) % RING) for i in range(RING)]
DOWN = [(i, (i - 1) % RING) for i in range(RING)]
SWAP = [(0, 1), (1, 0)]

TN = (((0,), (0,)), ((), ()))
HBM = pl.BlockSpec(memory_space=pltpu.HBM)
VMEM = pl.BlockSpec(memory_space=pltpu.VMEM)
SMEM = pl.BlockSpec(memory_space=pltpu.SMEM)


def merge_kernel(odd, train, low, high, main, half, total):
    total[...] = train[...].astype(jnp.float32) + mix_rate * lax.dot_general(
        low[...], high[...], TN, preferred_element_type=jnp.float32
    )
    size = half.shape[0]
    rows = total.shape[0]
    start = pl.multiple_of(odd[0] * size, size)
    rest = pl.multiple_of((1 - odd[0]) * (rows - size), size)
    main[...] = total[pl.ds(start, rows - size), :].astype(jnp.bfloat16).T
    half[...] = total[pl.ds(rest, size), :].astype(jnp.bfloat16)


def merge(odd, train, low, high):
    rows, cols = train.shape
    size = rows % 128
    return pl.pallas_call(
        merge_kernel,
        out_shape=(
            jax.ShapeDtypeStruct((cols, rows - size), jnp.bfloat16),
            jax.ShapeDtypeStruct((size, cols), jnp.bfloat16),
        ),
        in_specs=[SMEM, VMEM, VMEM, VMEM],
        out_specs=(VMEM, VMEM),
        scratch_shapes=[pltpu.VMEM((rows, cols), jnp.float32)],
    )(odd, train, low.T, high)


def merge_down_kernel(train, high, low, gate, up, out):
    rows, size = train.shape[0], gate.shape[0]
    out[:rows, :] = (
        train[...].astype(jnp.float32)
        + mix_rate * lax.dot_general(high[...], low[...], TN, preferred_element_type=jnp.float32)
    ).astype(jnp.bfloat16)
    out[rows : rows + size, :] = gate[...]
    out[rows + size :, :] = up[...]


def merge_down(train, low, high, gate, up):
    rows = train.shape[1] + 2 * gate.shape[0]
    return pl.pallas_call(
        merge_down_kernel,
        out_shape=jax.ShapeDtypeStruct((rows, train.shape[0]), jnp.bfloat16),
        in_specs=[VMEM] * 5,
        out_specs=VMEM,
    )(train.T, high, low.T, gate, up)


def place(offsets, blocks, outs, shapes, axis):
    fresh = outs is None
    count = len(blocks)

    def kernel(at, *refs):
        sources = refs[:count]
        targets = refs[count if fresh else count + len(shapes) :][: len(shapes)]
        sems = refs[-1]
        copies = []
        for i, (_, which, first, rows, base) in enumerate(blocks):
            source = sources[i].at[pl.ds(first, rows), :]
            if axis == 1:
                begin = pl.multiple_of(at[i] * 128, 128)
                target = targets[which].at[pl.ds(base, rows), pl.ds(begin, sources[i].shape[1])]
            else:
                begin = pl.multiple_of(at[i] * 64 + base, 32)
                target = targets[which].at[pl.ds(begin, rows), :]
            copies.append(pltpu.make_async_copy(source, target, sems.at[i]))
        for copy in copies:
            copy.start()
        for copy in copies:
            copy.wait()

    return pl.pallas_call(
        kernel,
        out_shape=tuple(jax.ShapeDtypeStruct(s, jnp.bfloat16) for s in shapes),
        in_specs=[SMEM] + [VMEM] * count + ([] if fresh else [HBM] * len(shapes)),
        out_specs=tuple(HBM for _ in shapes),
        scratch_shapes=[pltpu.SemaphoreType.DMA((count,))],
        input_output_aliases={} if fresh else {1 + count + i: i for i in range(len(shapes))},
    )(offsets, *[b[0] for b in blocks], *(() if fresh else outs))


def place_last_kernel(
    split, size, at, own, left, right, far_top, far_low, _g, _u, _d, gate, up, down, turned, store, whole
):
    rows = down.shape[0] // 8
    odd = at[0]
    base = pl.multiple_of(at[1] * 64, 64)
    copies = [
        pltpu.make_async_copy(far_top, down.at[pl.ds(base, split), :], whole.at[0]),
        pltpu.make_async_copy(
            far_low.at[pl.ds(0, rows - split), :],
            down.at[pl.ds(pl.multiple_of(base + split, 32), rows - split), :],
            whole.at[1],
        ),
    ]
    for copy in copies:
        copy.start()

    def turn(is_odd):
        mate, other = (left, right) if is_odd else (right, left)
        inner, outer = (own, rows), (far_low, rows - split)
        for k, (x, other_x) in enumerate(((inner, (mate, rows)), (outer, (other, rows)))):
            parts = (other_x, x) if is_odd else (x, other_x)
            for which in range(2):
                both = [ref[first + which * size : first + (which + 1) * size, :] for ref, first in parts]
                turned[k * 2 + which] = jnp.concatenate(both, axis=0).T

    for is_odd in (False, True):

        @pl.when(odd == int(is_odd))
        def _():
            turn(is_odd)

    stores = []
    for k in range(2):
        begin = pl.multiple_of(at[2 + k] * 128, 128)
        for which, out in enumerate((gate, up)):
            copy = pltpu.make_async_copy(
                turned.at[k * 2 + which], out.at[:, pl.ds(begin, 2 * size)], store.at[k * 2 + which]
            )
            copy.start()
            stores.append(copy)
    for copy in copies + stores:
        copy.wait()


def place_last(scalars, own, left, right, far_top, far_low, outs):
    split = far_top.shape[0]
    rows = outs[2].shape[0] // 8
    size = (own.shape[0] - rows) // 2
    cols = own.shape[1]
    return pl.pallas_call(
        functools.partial(place_last_kernel, split, size),
        out_shape=tuple(jax.ShapeDtypeStruct(o.shape, o.dtype) for o in outs),
        in_specs=[SMEM] + [VMEM] * 5 + [HBM] * 3,
        out_specs=(HBM, HBM, HBM),
        scratch_shapes=[
            pltpu.VMEM((4, cols, 2 * size), jnp.bfloat16),
            pltpu.SemaphoreType.DMA((4,)),
            pltpu.SemaphoreType.DMA((2,)),
        ],
        input_output_aliases={6: 0, 7: 1, 8: 2},
    )(scalars, own, left, right, far_top, far_low, *outs)


def local(
    train_gate,
    low_gate,
    high_gate,
    train_up,
    low_up,
    high_up,
    train_down,
    low_down,
    high_down,
    norm_train,
    norm_step,
):
    zh, y = lax.axis_index("zh"), lax.axis_index("y")
    odd = lax.rem(y, 2)
    tall = (low_down.shape[0], 8 * train_gate.shape[0])
    wide = (8 * train_down.shape[1], train_down.shape[0])

    def both(x):
        return lax.ppermute(x, "y", UP), lax.ppermute(x, "y", DOWN)

    def relay(pair, half):
        left, right = pair
        return lax.ppermute(left[:half], "y", UP), lax.ppermute(right[half:], "y", DOWN)

    A, half_gate = merge(odd[None], train_gate, low_gate, high_gate)
    yA = both(A)
    zA = lax.ppermute(A, "zh", SWAP)
    B, half_up = merge(odd[None], train_up, low_up, high_up)
    yB = both(B)
    C = merge_down(train_down, low_down, high_down, half_gate, half_up)
    yC = both(C)
    zB = lax.ppermute(B, "zh", SWAP)
    zC = lax.ppermute(C, "zh", SWAP)
    hA, hC = A.shape[0] // 2, C.shape[0] // 2
    fA, fB, fC = relay(yA, hA), relay(yB, hA), relay(yC, hC)
    wA, wB, wC = both(zA), both(zB), both(zC)
    oA = lax.ppermute(fA[0], "zh", SWAP), lax.ppermute(fA[1], "zh", SWAP)
    gB, gC = relay(wB, hA), relay(wC, hC)

    spots = [lax.rem(y + k, 4) for k in (0, 3, 1, 2)]

    def index(half):
        return [half * 4 + s for s in spots]

    def columns(half):
        return [(r // 2) * 7 + (r % 2) * 4 for r in index(half)]

    def near(own, pair, half, which, outs, shapes):
        blocks = [(x, which, 0, x.shape[0], 0) for x in (own, *pair)]
        return place(jnp.stack(columns(half)[:3]), blocks, outs, shapes, 1)

    halves = (zh, 1 - zh)
    gate = near(A, yA, halves[0], 0, None, (tall,))
    up = near(B, yB, halves[0], 0, None, (tall,))
    rows = wide[0] // 8

    def near_down(own, pair, half, outs):
        at = jnp.stack(index(half)[:3]) * (rows // 64)
        return place(at, [(x, 0, 0, rows, 0) for x in (own, *pair)], outs, (wide,), 0)

    down = near_down(C, yC, halves[0], None)

    def scalars(half):
        r = index(half)
        return jnp.stack([odd, r[3] * (rows // 64), (r[0] // 2) * 7 + 3, (r[3] // 2) * 7 + 3])

    def far(pair, half, outs):
        col = columns(half)[3]
        blocks = [(pair[0], 0, 0, hA, 0), (pair[1], 0, 0, hA, hA)]
        return place(jnp.stack([col, col]), blocks, outs, (tall,), 1)

    (gate,) = far(fA, halves[0], gate)
    (up,) = far(fB, halves[0], up)
    gate, up, down = place_last(scalars(halves[0]), C, *yC, *fC, (gate, up, *down))
    (gate,) = near(zA, wA, halves[1], 0, (gate,), (tall,))
    (down,) = near_down(zC, wC, halves[1], (down,))
    (up,) = near(zB, wB, halves[1], 0, (up,), (tall,))
    (gate,) = far(oA, halves[1], (gate,))
    gate, up, down = place_last(scalars(halves[1]), zC, *wC, *gC, (gate, up, down))
    (up,) = far(gB, halves[1], (up,))

    share = norm_train.shape[0]
    column = (lax.axis_index("zl") * 2 + lax.axis_index("xl")) * 2 + lax.axis_index("core")
    norm = lax.dynamic_update_slice(
        jnp.zeros((share * 128,), jnp.bfloat16),
        (norm_train + norm_step).astype(jnp.bfloat16),
        (((zh * 4 + y) * 16 + column) * share,),
    )
    for axis, flip in (("core", 1), ("xl", 1), ("y", 1), ("zl", 1), ("y", 2), ("zl", 2), ("zh", 1)):
        n = lax.axis_size(axis)
        norm = norm + lax.ppermute(norm, axis, [(i, i ^ flip) for i in range(n)])
    return gate, up, down, norm


def solution(mesh):
    finer = Mesh(
        mesh.devices.reshape(2, 4, 4, 2, 2, mesh.shape["shift"]),
        (*ROWS, *COLS, "shift"),
    )
    return jax.shard_map(
        local,
        mesh=finer,
        in_specs=(
            P(("shift", *ROWS), COLS),
            P(("shift", *ROWS), None),
            P("shift", COLS),
            P(("shift", *ROWS), COLS),
            P(("shift", *ROWS), None),
            P("shift", COLS),
            P(("shift", *COLS), ROWS),
            P(("shift", *COLS), None),
            P("shift", ROWS),
            P(("shift", *ROWS, *COLS)),
            P(("shift", *ROWS, *COLS)),
        ),
        out_specs=(P(("shift", *COLS), None), P(("shift", *COLS), None), P("shift", COLS), P("shift")),
        check_vma=False,
    )
```

```python
import functools

import jax
import jax.numpy as jnp
from jax import lax
from jax.experimental import pallas as pl
from jax.experimental.pallas import tpu as pltpu
from jax.sharding import Mesh
from jax.sharding import PartitionSpec as P

ROWS = ("zh", "y")
COLS = ("zl", "xl", "core")
mix_rate = 1.0


RING = 4
FULL = 384
UP = [(i, (i + 1) % RING) for i in range(RING)]
DOWN = [(i, (i - 1) % RING) for i in range(RING)]
SWAP = [(0, 1), (1, 0)]

HBM = pl.BlockSpec(memory_space=pltpu.HBM)
VMEM = pl.BlockSpec(memory_space=pltpu.VMEM)
LIMIT = pltpu.CompilerParams(vmem_limit_bytes=8 * 1024 * 1024)
SMEM = pl.BlockSpec(memory_space=pltpu.SMEM)


def split_kernel(alone, at, whole, *refs):
    rows = whole.shape[0]
    size = rows % 128
    full = rows - size
    odd = lax.rem(at[1], 2)
    start = pl.multiple_of(odd * size, size)
    rest = pl.multiple_of((1 - odd) * full, size)
    if alone:
        main, half = refs
        main[...] = whole[pl.ds(start, full), :].T
        half[...] = whole[pl.ds(rest, size), :]
        return
    gate, main = refs
    main[:, :full] = whole[pl.ds(start, full), :].T
    pair = (gate[...], whole[pl.ds(rest, size), :])
    for is_odd in (False, True):

        @pl.when(odd == int(is_odd))
        def _():
            main[:, full:] = jnp.concatenate(pair[::-1] if is_odd else pair, axis=0).T


def split(at, whole, gate=None):
    rows, cols = whole.shape
    size = rows % 128
    if gate is None:
        shapes = ((cols, rows - size), (size, cols))
    else:
        shapes = ((cols, rows + size),)
    return pl.pallas_call(
        functools.partial(split_kernel, gate is None),
        out_shape=tuple(jax.ShapeDtypeStruct(x, jnp.bfloat16) for x in shapes),
        in_specs=[SMEM, VMEM] + ([] if gate is None else [VMEM]),
        out_specs=tuple(VMEM for _ in shapes),
        compiler_params=LIMIT,
    )(at, whole, *(() if gate is None else (gate,)))


def merge(train, low, high):
    update = jnp.dot(low, high, preferred_element_type=jnp.float32)
    return (train.astype(jnp.float32) + mix_rate * update).astype(jnp.bfloat16)


def place(at, other, blocks, outs, shapes, pairs=None):
    names = tuple(shapes)
    fresh = outs is None
    count = len(blocks)
    arrays = [b[0] for b in blocks] + (list(pairs) if pairs else [])
    total = len(arrays)
    share = shapes["down"][0] // 8 if "down" in shapes else None

    def kernel(at_ref, *refs):
        sources = refs[:total]
        first = total if fresh else total + len(names)
        targets = dict(zip(names, refs[first : first + len(names)]))
        sems = refs[first + len(names)]
        zh, y = at_ref[0], at_ref[1]
        half = 4 * (1 - zh) if other else 4 * zh

        def spot(step):
            return half + lax.rem(y + step, 4)

        copies = []
        for i, (array, which, step, base) in enumerate(blocks):
            rows = array.shape[0]
            r = spot(step)
            if which == "down":
                source = sources[i]
                target = targets[which].at[pl.ds(pl.multiple_of(r * share + base, 32), rows), :]
            else:
                source = sources[i].at[:, pl.ds(0, FULL)]
                begin = pl.multiple_of(((r // 2) * 7 + lax.rem(r, 2) * 4) * 128, 128)
                target = targets[which].at[pl.ds(base, rows), pl.ds(begin, FULL)]
            copies.append(pltpu.make_async_copy(source, target, sems.at[i]))
        for copy in copies:
            copy.start()

        if pairs:
            turned, store = refs[first + len(names) + 1 :]
            own, left, right, far_top, far_low = sources[count:]
            odd = lax.rem(y, 2)
            rows = far_top.shape[0]

            def tile(ref, row):
                return ref[row : row + rows, FULL:].astype(jnp.float32)

            def join(is_odd):
                mate, rest = (left, right) if is_odd else (right, left)
                front = lax.broadcasted_iota(jnp.int32, (rows, 128), 1) < 64
                for part, far in enumerate((far_top, far_low)):
                    row = part * rows
                    for k, two in enumerate((((own, row), (mate, row)), ((far, 0), (rest, row)))):
                        even, uneven = [tile(*x) for x in (two[::-1] if is_odd else two)]
                        gate = jnp.where(front, even, uneven)
                        up = pltpu.roll(jnp.where(front, uneven, even), 64, 1)
                        turned[k * 2, row : row + rows, :] = gate.astype(jnp.bfloat16)
                        turned[k * 2 + 1, row : row + rows, :] = up.astype(jnp.bfloat16)

            for is_odd in (False, True):

                @pl.when(odd == int(is_odd))
                def _():
                    join(is_odd)

            for k, step in enumerate((0, 2)):
                begin = pl.multiple_of(((spot(step) // 2) * 7 + 3) * 128, 128)
                for u, which in enumerate(("gate", "up")):
                    n = k * 2 + u
                    target = targets[which].at[:, pl.ds(begin, 128)]
                    copy = pltpu.make_async_copy(turned.at[n], target, store.at[n])
                    copy.start()
                    copies.append(copy)
        for copy in copies:
            copy.wait()

    scratch = [pltpu.SemaphoreType.DMA((count,))]
    if pairs:
        scratch += [pltpu.VMEM((4, pairs[0].shape[0], 128), jnp.bfloat16), pltpu.SemaphoreType.DMA((4,))]
    return pl.pallas_call(
        kernel,
        out_shape=tuple(jax.ShapeDtypeStruct(shapes[n], jnp.bfloat16) for n in names),
        in_specs=[SMEM] + [VMEM] * total + ([] if fresh else [HBM] * len(names)),
        out_specs=tuple(HBM for _ in names),
        scratch_shapes=scratch,
        input_output_aliases={} if fresh else {1 + total + i: i for i in range(len(names))},
        compiler_params=LIMIT,
    )(at, *arrays, *(() if fresh else outs))


def local(
    train_gate,
    low_gate,
    high_gate,
    train_up,
    low_up,
    high_up,
    train_down,
    low_down,
    high_down,
    norm_train,
    norm_step,
):
    zh, y = lax.axis_index("zh"), lax.axis_index("y")
    at = jnp.stack([zh, y])
    tall = (low_down.shape[0], 8 * train_gate.shape[0])
    wide = (8 * train_down.shape[1], train_down.shape[0])

    def both(x):
        return lax.ppermute(x, "y", UP), lax.ppermute(x, "y", DOWN)

    def relay(pair):
        left, right = pair
        half = left.shape[0] // 2
        return lax.ppermute(left[:half], "y", UP), lax.ppermute(right[half:], "y", DOWN)

    D = merge(train_down, low_down, high_down).T
    yD = both(D)
    zD = lax.ppermute(D, "zh", SWAP)
    A, half = split(at, merge(train_gate, low_gate, high_gate))
    yA = both(A)
    (B,) = split(at, merge(train_up, low_up, high_up), half)
    yB = both(B)
    zB = lax.ppermute(B, "zh", SWAP)
    zA = lax.ppermute(A, "zh", SWAP)
    fD, fA, fB = relay(yD), relay(yA), relay(yB)
    wD, wB, wA = both(zD), both(zB), both(zA)
    gD, gB = relay(wD), relay(wB)
    oA = lax.ppermute(fA[0], "zh", SWAP), lax.ppermute(fA[1], "zh", SWAP)

    def near(which, own, pair):
        return [(x, which, step, 0) for x, step in zip((own, *pair), (0, 3, 1)) if x is not None]

    def far(which, pair):
        return [(pair[0], which, 2, 0), (pair[1], which, 2, pair[0].shape[0])]

    shapes = {"gate": tall, "up": tall, "down": wide}

    def only(*which):
        return {n: shapes[n] for n in which}

    down, gate = place(at, False, near("down", D, yD) + near("gate", A, yA), None, only("down", "gate"))
    (up,) = place(at, False, near("up", B, yB), None, only("up"))
    gate, up, down = place(
        at, False, far("down", fD) + far("gate", fA) + far("up", fB), (gate, up, down), shapes, (B, *yB, *fB)
    )
    (down,) = place(at, True, near("down", zD, wD), (down,), only("down"))
    (up,) = place(at, True, near("up", zB, wB), (up,), only("up"))
    gate, up, down = place(
        at,
        True,
        far("down", gD) + far("up", gB) + near("gate", zA, (None, None)),
        (gate, up, down),
        shapes,
        (zB, *wB, *gB),
    )
    (gate,) = place(at, True, near("gate", None, wA) + far("gate", oA), (gate,), only("gate"))

    count = norm_train.shape[0]
    column = (lax.axis_index("zl") * 2 + lax.axis_index("xl")) * 2 + lax.axis_index("core")
    norm = lax.dynamic_update_slice(
        jnp.zeros((count * 128,), jnp.bfloat16),
        (norm_train + norm_step).astype(jnp.bfloat16),
        (((zh * 4 + y) * 16 + column) * count,),
    )
    for axis, flip in (("zl", 1), ("zl", 2), ("y", 1), ("y", 2), ("core", 1), ("xl", 1), ("zh", 1)):
        came = lax.ppermute(norm, axis, [(i, i ^ flip) for i in range(lax.axis_size(axis))])
        norm = norm + came
    return gate, up, down, norm


def solution(mesh):
    finer = Mesh(
        mesh.devices.reshape(2, 4, 4, 2, 2, mesh.shape["shift"]),
        (*ROWS, *COLS, "shift"),
    )
    return jax.shard_map(
        local,
        mesh=finer,
        in_specs=(
            P(("shift", *ROWS), COLS),
            P(("shift", *ROWS), None),
            P("shift", COLS),
            P(("shift", *ROWS), COLS),
            P(("shift", *ROWS), None),
            P("shift", COLS),
            P(("shift", *COLS), ROWS),
            P(("shift", *COLS), None),
            P("shift", ROWS),
            P(("shift", *ROWS, *COLS)),
            P(("shift", *ROWS, *COLS)),
        ),
        out_specs=(P(("shift", *COLS), None), P(("shift", *COLS), None), P("shift", COLS), P("shift")),
        check_vma=False,
    )
```
